32 devices in a mesh: seq: 16 (over z, y, x), head: 2 (over core).
Axes of the slice: x: 2, y: 2, z: 4, core: 2. Of those that a mesh axis runs over, the one named last changes fastest.
Arguments:
- queries: bfloat16 [4096, 2048], P('seq', 'head'), may hold values from -0.5 to 0.5
- keys: bfloat16 [4096, 2048], P('seq', 'head'), may hold values from -0.5 to 0.5
- values: bfloat16 [4096, 4096], P('seq', 'head'), may hold values from -0.5 to 0.5
- out_grad: bfloat16 [4096, 4096], P('seq', 'head'), may hold values from -0.5 to 0.5
- log_gates: float32 [4096, 2048], P('seq', 'head'), may hold values from -1 to 0
- boundary_states: float32 [16, 16, 128, 256], P('seq', 'head'), may hold values from -6 to 6
- gate_up: float32 [16, 2048], P(None, 'head'), may hold values from -1.5 to 1.5
Outputs:
- query_grad: bfloat16 [4096, 2048], P('seq', 'head')
- key_gradient_rows: bfloat16 [4096, 2048], P('seq', 'head')
- value_grad: bfloat16 [4096, 4096], P('seq', 'head')
- gate_grad: float32 [4096, 2048], P('seq', 'head')
- latent_grad: float32 [16, 4096], P(None, 'seq')
The draws below stay inside these ranges and needn't reach their ends.
All inputs are finite; a program needn't handle non-finite values.
Results may differ from the reference program's by a relative error of at most 0.001.
Values sent between devices are 32-bit elements; how exact they have to be, the bound alone decides.
No kernel may reach another device: no remote copies, remote signals or barrier semaphores. Data moves between devices by JAX's collectives and lax.ppermute only.
A program may use at most 128 MiB of HBM per device.

```python
import jax
import jax.numpy as jnp
from jax import lax

HEADS = 16
DK = 128
DV = 256
RANK = 16
SPAN = 64
TOK_DEV = 256
SHARDS = 16
TOKENS = 4096


def draw_log_gates(key, part):
    streams = jax.random.split(jax.random.fold_in(key, 11), 6)
    channels = HEADS * DK
    fast_share = 0.5
    is_fast = jax.random.uniform(streams[0], (channels,), jnp.float32) < fast_share
    fast_rate = jnp.exp(jax.random.uniform(streams[1], (channels,), jnp.float32, jnp.log(1.0 / 50.0), jnp.log(1.0 / 30.0)))
    slow_rate = 0.4 / TOKENS
    base = jnp.where(is_fast, fast_rate, slow_rate)
    shard_factor = jnp.exp(jax.random.uniform(streams[2], (SHARDS, 1, channels), jnp.float32, -0.7, 0.7))
    rough = jax.random.uniform(streams[3], (SHARDS, TOK_DEV, channels), jnp.float32, 0.5, 1.5)
    decay_speeds = (base[None, None, :] * shard_factor * rough).reshape(TOKENS, channels)
    places = jax.random.randint(streams[4], (3,), 0, TOKENS)
    masked_out = jnp.any(jnp.arange(TOKENS)[:, None] == places[None, :], axis=1)
    objective_value = jax.random.uniform(streams[5], (channels,), jnp.float32, 0.2, 0.4)
    shard_outburst = -jnp.log(1.0 - objective_value)
    return -(decay_speeds + jnp.where(masked_out[:, None], shard_outburst[None, :], 0.0))


def steps_of(own_key, shape, shards, least, largest):
    loudness = 1.0
    for dim, shards_of in shards:
        steps = jax.random.uniform(jax.random.fold_in(jax.random.fold_in(own_key, 6), dim), (shards_of,), jnp.float32, least / len(shards), largest / len(shards))
        loudness = loudness * jnp.repeat(jnp.exp(steps), shape[dim] // shards_of).reshape((-1,) + (1,) * (len(shape) - 1 - dim))
    return loudness


def gaussian(stream_key, shape, scale, limit, shards=(), kind=jnp.bfloat16):
    level = steps_of(stream_key, shape, shards, -0.22, 0.18) if shards else 1.0
    array = jax.random.normal(stream_key, shape, jnp.float32) * scale * level
    return jnp.minimum(jnp.maximum(array, -limit), limit).astype(kind)


def setup_inputs(seed: int = 0) -> dict:
    key_of = jax.random.split(jax.random.key(seed), 8)
    return {
        "queries": gaussian(key_of[0], (TOKENS, HEADS * DK), 0.08, 0.5, ((0, 16), (1, 2))),
        "keys": gaussian(key_of[1], (TOKENS, HEADS * DK), 0.08, 0.5, ((0, 16), (1, 2))),
        "values": gaussian(key_of[2], (TOKENS, HEADS * DV), 0.08, 0.5, ((0, 16), (1, 2))),
        "out_grad": gaussian(key_of[3], (TOKENS, HEADS * DV), 0.08, 0.5, ((0, 16), (1, 2))),
        "log_gates": draw_log_gates(jax.random.fold_in(key_of[7], 71), 0),
        "boundary_states": gaussian(key_of[5], (SHARDS, HEADS, DK, DV), 1.0, 6.0, ((0, 16), (1, 2)), jnp.float32),
        "gate_up": gaussian(key_of[6], (RANK, HEADS * DK), RANK ** -0.5, 1.5, ((1, 2),), jnp.float32),
    }


highest = lax.Precision.HIGHEST


def one_head(inputs):
    queries, keys, values, out_grad, log_gates, entering, gate_up = inputs
    blocks = TOKENS // SPAN
    per_shard = TOK_DEV // SPAN
    query_blocks = queries.reshape(blocks, SPAN, DK)
    key_blocks = keys.reshape(blocks, SPAN, DK)
    value_blocks = values.reshape(blocks, SPAN, DV)
    grad_blocks = out_grad.reshape(blocks, SPAN, DV)
    within = jnp.cumsum(log_gates.reshape(blocks, SPAN, DK), axis=1)
    block_sum = within[:, -1]
    query_up = query_blocks * jnp.exp(within)
    key_down = key_blocks * jnp.exp(-within)
    key_end = key_blocks * jnp.exp(block_sum[:, None] - within)

    def forward(current, carried_in):
        position, decays, key_piece, value_piece = carried_in
        opening = jnp.where(position % per_shard == 0, entering[position // per_shard], current)
        following = jnp.exp(decays)[:, None] * opening + jnp.dot(key_piece.T, value_piece, precision=highest)
        return following, opening

    _, states = lax.scan(forward, jnp.zeros((DK, DV), jnp.float32),
                         (jnp.arange(blocks, dtype=jnp.int32), block_sum, key_end, value_blocks))

    def backward(next_grad, carried_in):
        decays, query_piece, grad_piece = carried_in
        preceding_shards = jnp.exp(decays)[:, None] * next_grad + jnp.dot(query_piece.T, grad_piece, precision=highest)
        return preceding_shards, next_grad

    _, end_grads = lax.scan(backward, jnp.zeros((DK, DV), jnp.float32), (block_sum, query_up, grad_blocks), reverse=True)
    row_index = jnp.arange(SPAN, dtype=jnp.int32)[:, None]
    col_index = jnp.arange(SPAN, dtype=jnp.int32)[None, :]
    causal = (col_index <= row_index).astype(jnp.float32)
    scores = jnp.einsum("cti,csi->cts", query_up, key_down, precision=highest) * causal
    grad_dots = jnp.einsum("ctj,csj->cts", grad_blocks, value_blocks, precision=highest) * causal
    query_grad = jnp.exp(within) * (jnp.einsum("ctj,cij->cti", grad_blocks, states, precision=highest)
                                    + jnp.einsum("cts,csi->cti", grad_dots, key_down, precision=highest))
    key_gradient_rows = (jnp.exp(-within) * jnp.einsum("cst,csi->cti", grad_dots, query_up, precision=highest)
                + jnp.exp(block_sum[:, None] - within) * jnp.einsum("ctj,cij->cti", value_blocks, end_grads, precision=highest))
    value_grad = (jnp.einsum("cst,csj->ctj", scores, grad_blocks, precision=highest)
                  + jnp.einsum("cti,cij->ctj", key_end, end_grads, precision=highest))
    gate_terms = (query_blocks * query_grad - key_blocks * key_gradient_rows).reshape(TOKENS, DK)
    gate_grad = jnp.flip(jnp.cumsum(jnp.flip(gate_terms, 0), axis=0), 0)
    softness = (1.0 - jnp.exp(16.0 * log_gates)) / 16.0
    latent = jnp.dot(gate_up, (gate_grad * softness).T, precision=highest)
    return (query_grad.reshape(TOKENS, DK), key_gradient_rows.reshape(TOKENS, DK), value_grad.reshape(TOKENS, DV),
            gate_grad, latent)


def heads_first(matrix, channels):
    return matrix.astype(jnp.float32).reshape(TOKENS, HEADS, channels).transpose(1, 0, 2)


def tokens_first(matrix, channels):
    return matrix.transpose(1, 0, 2).reshape(TOKENS, HEADS * channels)


def reference(queries, keys, values, out_grad, log_gates, boundary_states, gate_up):
    stacked = (heads_first(queries, DK), heads_first(keys, DK), heads_first(values, DV),
               heads_first(out_grad, DV), heads_first(log_gates, DK),
               boundary_states.transpose(1, 0, 2, 3),
               gate_up.reshape(RANK, HEADS, DK).transpose(1, 0, 2))
    query_grad, key_gradient_rows, value_grad, gate_grad, latent = lax.map(one_head, stacked)
    return (tokens_first(query_grad, DK).astype(jnp.bfloat16),
            tokens_first(key_gradient_rows, DK).astype(jnp.bfloat16),
            tokens_first(value_grad, DV).astype(jnp.bfloat16),
            tokens_first(gate_grad, DK),
            jnp.sum(latent, axis=0))
```

```python
import functools
import math

import jax
import jax.numpy as jnp
from jax import lax
from jax.experimental import pallas as pl
from jax.experimental.pallas import tpu as pltpu
from jax.sharding import PartitionSpec as P

CHUNK = 128
TEAM = 8
PAD = 8

f32 = jnp.float32
bf16 = jnp.bfloat16


def dot(a, b, da, db):
    return lax.dot_general(a, b, (((da,), (db,)), ((), ())), preferred_element_type=f32)


def split(x):
    hi = x.astype(bf16)
    return hi, (x - hi.astype(f32)).astype(bf16)


def halves(x):
    width = x.shape[1] // 2
    return x[:, :width] + x[:, width:]


def at_or_after(rows, cols):
    return lax.broadcasted_iota(jnp.int32, (rows, cols), 0) >= lax.broadcasted_iota(jnp.int32, (rows, cols), 1)


def at_or_before(rows, cols):
    return lax.broadcasted_iota(jnp.int32, (rows, cols), 0) <= lax.broadcasted_iota(jnp.int32, (rows, cols), 1)


def running_sum(g):
    count = g.shape[0]
    lower = jnp.where(at_or_after(count, count), 1.0, 0.0).astype(bf16)
    return halves(dot(lower, jnp.concatenate(split(g), axis=1), 1, 0))


def later_sum(g):
    count = g.shape[0]
    upper = jnp.where(at_or_before(count, count), 1.0, 0.0).astype(bf16)
    return halves(dot(upper, jnp.concatenate(split(g), axis=1), 1, 0))


def opening_kernel(team, parts, place_ref, g_ref, q_ref, do_ref, *outs):
    head = pl.program_id(0)
    per_owner = outs[0].shape[0]
    sub = outs[0].shape[1] - PAD
    total = running_sum(g_ref[...])
    up = jnp.concatenate(split(q_ref[...].astype(f32) * jnp.exp(total)), axis=1)
    grad = halves(dot(do_ref[...], up, 0, 0))
    decay = jnp.broadcast_to(jnp.exp(total[-1:]), (PAD, total.shape[1]))
    for part in range(parts):
        unit = head * parts + part
        slot = (unit // per_owner) ^ place_ref[0]
        inner = unit % per_owner
        for number in range(team):

            @pl.when(slot == number)
            def _():
                outs[number][inner, :sub] = grad[part * sub : (part + 1) * sub]
                outs[number][inner, sub:] = decay


def local_kernel(g_ref, q_ref, k_ref, v_ref, do_ref, s_ref, dq_ref, dk_ref, dv_ref, terms_ref, fading_ref):
    length = g_ref.shape[0]
    total = running_sum(g_ref[...])
    q = q_ref[...].astype(f32)
    k = k_ref[...].astype(f32)
    v = v_ref[...]
    do = do_ref[...]
    from_state = halves(dot(do, jnp.concatenate(split(s_ref[0, 0]), axis=0), 1, 1))
    dq_all = jnp.exp(total) * from_state
    dots = split(jnp.where(at_or_after(length, length), dot(do, v, 1, 1), 0.0))
    flipped = split(jnp.where(at_or_before(length, length), dot(v, do, 1, 1), 0.0))
    dq = []
    dk = [0.0] * (length // CHUNK)
    dv = [0.0] * (length // CHUNK)
    for number in range(length // CHUNK):
        start, end = number * CHUNK, (number + 1) * CHUNK
        middle = total[start + CHUNK // 2 - 1 : start + CHUNK // 2]
        grow = jnp.exp(total[start:end] - middle)
        fade = jnp.exp(middle - total[:end])
        q_hi, q_lo = split(q[start:end] * grow)
        k_hi, k_lo = split(k[:end] * fade)
        dq.append(
            dq_all[start:end]
            + grow
            * (
                halves(dot(dots[0][start:end, :end], jnp.concatenate([k_hi, k_lo], axis=1), 1, 0))
                + dot(dots[1][start:end, :end], k_hi, 1, 0)
            )
        )
        dk_more = fade * (
            halves(dot(flipped[0][:end, start:end], jnp.concatenate([q_hi, q_lo], axis=1), 1, 0))
            + dot(flipped[1][:end, start:end], q_hi, 1, 0)
        )
        scores = dot(jnp.concatenate([k_hi, k_lo], axis=1), jnp.concatenate([q_hi, q_hi], axis=1), 1, 1)
        scores = scores + dot(k_hi, q_lo, 1, 1)
        seen = lax.broadcasted_iota(jnp.int32, (end, CHUNK), 0) <= start + lax.broadcasted_iota(
            jnp.int32, (end, CHUNK), 1
        )
        pair = jnp.concatenate(split(jnp.where(seen, scores, 0.0)), axis=1)
        dv_more = dot(pair, jnp.concatenate([do[start:end], do[start:end]], axis=0), 1, 0)
        for early in range(number + 1):
            rows = slice(early * CHUNK, (early + 1) * CHUNK)
            dk[early] = dk[early] + dk_more[rows]
            dv[early] = dv[early] + dv_more[rows]
    dq = jnp.concatenate(dq, axis=0)
    dk = jnp.concatenate(dk, axis=0)
    dq_ref[...] = dq.astype(bf16)
    dk_ref[...] = dk
    dv_ref[...] = jnp.concatenate(dv, axis=0)
    terms_ref[...] = q * dq - k * dk
    fading_ref[...] = jnp.exp(total[-1:] - total)


def team_total_kernel(team, place_ref, *refs):
    pieces, out_ref = refs[:team], refs[team]
    sub = out_ref.shape[1] - PAD
    for place in range(team):

        @pl.when(place_ref[0] == place)
        def _():
            order = [pieces[member ^ place] for member in range(team)]
            for inner in range(out_ref.shape[0]):
                decays = [ref[inner, sub:] for ref in order]
                whole = decays[0]
                for decay in decays[1:]:
                    whole = whole * decay
                out_ref[inner, sub:] = whole

                def rows(step, _):
                    at = pl.ds(pl.multiple_of(step * PAD, PAD), PAD)
                    state = order[-1][inner, at]
                    for ref, decay in zip(order[-2::-1], decays[-2::-1]):
                        state = ref[inner, at] + decay * state
                    out_ref[inner, at] = state
                    return 0

                lax.fori_loop(0, sub // PAD, rows, 0, unroll=4)


def team_carry_kernel(team, place_ref, *refs):
    pieces, behind_ref, outs = refs[:team], refs[team], refs[team + 1 :]
    sub = outs[0].shape[1]
    for place in range(team):

        @pl.when(place_ref[0] == place)
        def _():
            order = [pieces[member ^ place] for member in range(team)]
            targets = [outs[member ^ place] for member in range(team)]
            for inner in range(outs[0].shape[0]):
                decays = [ref[inner, sub:] for ref in order]

                def rows(step, _):
                    at = pl.ds(pl.multiple_of(step * PAD, PAD), PAD)
                    state = behind_ref[inner, at]
                    for member in range(team - 1, -1, -1):
                        targets[member][inner, at] = state
                        if member:
                            state = order[member][inner, at] + decays[member] * state
                    return 0

                lax.fori_loop(0, sub // PAD, rows, 0, unroll=4)


def key_kernel(team, parts, place_ref, k_ref, v_ref, dk_ref, terms_ref, fading_ref, *refs):
    pieces, (out_ref, gate_ref, sum_ref, carry_ref), state_ref = refs[:team], refs[team:-1], refs[-1]
    head = pl.program_id(0)
    per_owner, sub = pieces[0].shape[:2]

    @pl.when(head == 0)
    def _():
        for number in range(team):
            owner = place_ref[0] ^ number
            state_ref[pl.ds(owner * per_owner, per_owner)] = pieces[number][...]

    state = jnp.concatenate([state_ref[head * parts + part] for part in range(parts)], axis=0)
    carry_ref[0] = state
    more = fading_ref[...] * halves(dot(v_ref[...], jnp.concatenate(split(state), axis=1), 1, 0))
    out_ref[...] = (dk_ref[...] + more).astype(bf16)
    terms = terms_ref[...] - k_ref[...].astype(f32) * more
    gate_ref[...] = terms
    sum_ref[...] = jnp.sum(terms, axis=0, keepdims=True)


def value_kernel(k_ref, fading_ref, carry_ref, dv_ref, gate_ref, out_ref, later_ref):
    s_hi, s_lo = split(carry_ref[0])
    k_hi, k_lo = split(k_ref[...].astype(f32) * fading_ref[...])
    more = dot(jnp.concatenate([k_hi, k_lo], axis=1), jnp.concatenate([s_hi, s_hi], axis=1), 1, 1)
    more = more + dot(k_hi, s_lo, 1, 1)
    out_ref[...] = (dv_ref[...] + more).astype(bf16)
    later_ref[...] = later_sum(gate_ref[...])


def gate_kernel(later_ref, behind_ref, g_ref, up_ref, gate_ref, latent_ref):
    grad = later_ref[...] + behind_ref[...]
    gate_ref[...] = grad
    x_hi, x_lo = split(grad * ((1.0 - jnp.exp(16.0 * g_ref[...])) / 16.0))
    u_hi, u_lo = split(up_ref[...])
    part = dot(u_hi, x_hi, 1, 1) + dot(u_hi, x_lo, 1, 1) + dot(u_lo, x_hi, 1, 1)

    @pl.when(pl.program_id(0) == 0)
    def _():
        latent_ref[...] = part

    @pl.when(pl.program_id(0) > 0)
    def _():
        latent_ref[...] += part


def whole(shape):
    return pl.BlockSpec(shape, lambda *_: (0,) * len(shape))


def struct(shape, dtype=f32):
    return jax.ShapeDtypeStruct(shape, dtype)


def call(kernel, grid, in_specs, out_specs, out_shape, flops, name, scratch=()):
    return pl.pallas_call(
        kernel,
        grid=grid,
        in_specs=in_specs,
        out_specs=out_specs,
        out_shape=out_shape,
        scratch_shapes=list(scratch),
        name=name,
        cost_estimate=pl.CostEstimate(flops=flops, bytes_accessed=4 * 1024 * 1024, transcendentals=0),
        compiler_params=pltpu.CompilerParams(dimension_semantics=("arbitrary",) * len(grid)),
    )


def exclusive_suffix(value, axis):
    count = lax.axis_size(axis)
    mine = lax.axis_index(axis)
    total, later = value, jnp.zeros_like(value)
    stride = 1
    while stride < count:
        perm = [(m, m ^ stride) for m in range(count)]
        other = lax.ppermute(total, axis, perm)
        later = jnp.where((mine & stride) == 0, later + other, later)
        total = total + other
        stride *= 2
    return later


def per_device(queries, keys, values, out_grad, log_gates, boundary_states, gate_up):
    count = lax.axis_size("seq")
    length, width = queries.shape
    _, heads, dk, dv = boundary_states.shape
    rank = gate_up.shape[0]
    team = math.gcd(TEAM, count)
    parts = team // math.gcd(heads, team)
    per_owner = heads * parts // team
    sub = dv // parts
    place = (lax.axis_index("seq") % team).astype(jnp.int32).reshape(1)
    smem = pl.BlockSpec(memory_space=pltpu.SMEM)
    narrow = pl.BlockSpec((length, dk), lambda h: (0, h))
    wide = pl.BlockSpec((length, dv), lambda h: (0, h))
    unit = 2 * length * dv * 256 * heads

    pieces = call(
        functools.partial(opening_kernel, team, parts),
        (heads,),
        [smem, narrow, narrow, wide],
        [whole((per_owner, sub + PAD, dk))] * team,
        [struct((per_owner, sub + PAD, dk))] * team,
        4 * unit,
        "opening",
    )(place, log_gates, queries, out_grad)

    query_grad, dk_part, dv_part, terms, fading = call(
        local_kernel,
        (heads,),
        [narrow, narrow, narrow, wide, wide, pl.BlockSpec((1, 1, dk, dv), lambda h: (0, h, 0, 0))],
        [narrow, narrow, wide, narrow, narrow],
        [
            struct((length, width), bf16),
            struct((length, width)),
            struct((length, heads * dv)),
            struct((length, width)),
            struct((length, width)),
        ],
        16 * unit,
        "local",
    )(log_gates, queries, keys, values, out_grad, boundary_states)

    def exchange(blocks):
        moved = [blocks[0]]
        for number in range(1, team):
            moved.append(lax.ppermute(blocks[number], "seq", [(m, m ^ number) for m in range(count)]))
        return moved

    pieces = exchange(pieces)
    piece = (per_owner, sub + PAD, dk)
    total = call(
        functools.partial(team_total_kernel, team),
        (1,),
        [smem] + [whole(piece)] * team,
        whole(piece),
        struct(piece),
        unit // 8,
        "team_total",
    )(place, *pieces)
    behind = lax.ppermute(total, "seq", [(m, m - team) for m in range(team, count)])
    step = 1
    while step < count // team - 1:
        further = lax.ppermute(behind, "seq", [(m, m - team * step) for m in range(team * step, count)])
        decay = behind[:, sub : sub + 1]
        behind = jnp.concatenate(
            [behind[:, :sub] + decay * further[:, :sub], behind[:, sub:] * further[:, sub:]], axis=1
        )
        step *= 2
    carries = call(
        functools.partial(team_carry_kernel, team),
        (1,),
        [smem] + [whole(piece)] * (team + 1),
        [whole((per_owner, sub, dk))] * team,
        [struct((per_owner, sub, dk))] * team,
        unit // 8,
        "team_carry",
    )(place, *pieces, behind)
    carries = exchange(carries)

    state_block = pl.BlockSpec((1, dv, dk), lambda h: (h, 0, 0))
    key_grad, gate_terms, sums, state = call(
        functools.partial(key_kernel, team, parts),
        (heads,),
        [smem, narrow, wide, narrow, narrow, narrow] + [whole((per_owner, sub, dk))] * team,
        [narrow, narrow, pl.BlockSpec((1, dk), lambda h: (0, h)), state_block],
        [
            struct((length, width), bf16),
            struct((length, width)),
            struct((1, width)),
            struct((heads, dv, dk)),
        ],
        2 * unit,
        "key",
        [pltpu.VMEM((heads * parts, sub, dk), f32)],
    )(place, keys, values, dk_part, terms, fading, *carries)

    value_grad, later = call(
        value_kernel,
        (heads,),
        [narrow, narrow, state_block, wide, narrow],
        [wide, narrow],
        [struct((length, heads * dv), bf16), struct((length, width))],
        4 * unit,
        "value",
    )(keys, fading, state, dv_part, gate_terms)

    behind_sum = exclusive_suffix(sums, "seq")
    gate_grad, latent = call(
        gate_kernel,
        (heads,),
        [narrow, pl.BlockSpec((1, dk), lambda h: (0, h)), narrow, pl.BlockSpec((rank, dk), lambda h: (0, h))],
        [narrow, whole((rank, length))],
        [struct((length, width)), struct((rank, length))],
        unit,
        "gate",
    )(later, behind_sum, log_gates, gate_up)
    if lax.axis_size("head") == 2:
        latent = latent + lax.ppermute(latent, "head", [(0, 1), (1, 0)])
    else:
        latent = lax.psum(latent, "head")
    return query_grad, key_grad, value_grad, gate_grad, latent


def solution(mesh):
    return jax.shard_map(
        per_device,
        mesh=mesh,
        in_specs=(
            P("seq", "head"),
            P("seq", "head"),
            P("seq", "head"),
            P("seq", "head"),
            P("seq", "head"),
            P("seq", "head", None, None),
            P(None, "head"),
        ),
        out_specs=(
            P("seq", "head"),
            P("seq", "head"),
            P("seq", "head"),
            P("seq", "head"),
            P(None, "seq"),
        ),
        check_vma=False,
    )
```

```python
import functools
import math

import jax
import jax.numpy as jnp
from jax import lax
from jax.experimental import pallas as pl
from jax.experimental.pallas import tpu as pltpu
from jax.sharding import PartitionSpec as P


CHUNK = 128
TEAM = 8
PAD = 8

f32 = jnp.float32
bf16 = jnp.bfloat16


def dot(a, b, da, db):
    return lax.dot_general(a, b, (((da,), (db,)), ((), ())), preferred_element_type=f32)


def split(x):
    hi = x.astype(bf16)
    return hi, (x - hi.astype(f32)).astype(bf16)


def halves(x):
    width = x.shape[1] // 2
    return x[:, :width] + x[:, width:]


def at_or_after(rows, cols):
    return lax.broadcasted_iota(jnp.int32, (rows, cols), 0) >= lax.broadcasted_iota(jnp.int32, (rows, cols), 1)


def at_or_before(rows, cols):
    return lax.broadcasted_iota(jnp.int32, (rows, cols), 0) <= lax.broadcasted_iota(jnp.int32, (rows, cols), 1)


def running_sum(g):
    count = g.shape[0]
    lower = jnp.where(at_or_after(count, count), 1.0, 0.0).astype(bf16)
    return halves(dot(lower, jnp.concatenate(split(g), axis=1), 1, 0))


def later_sum(g):
    count = g.shape[0]
    upper = jnp.where(at_or_before(count, count), 1.0, 0.0).astype(bf16)
    return halves(dot(upper, jnp.concatenate(split(g), axis=1), 1, 0))


def opening_kernel(team, parts, place_ref, g_ref, q_ref, do_ref, *refs):
    outs, grad_ref, decay_ref = refs[:team], refs[team], refs[team + 1]
    per_owner, rows, dk = outs[0].shape
    sub = rows - PAD
    heads = g_ref.shape[1] // dk
    dv = do_ref.shape[1] // heads
    for head in range(heads):
        keys = slice(head * dk, (head + 1) * dk)
        total = running_sum(g_ref[:, keys])
        up = jnp.concatenate(split(q_ref[:, keys].astype(f32) * jnp.exp(total)), axis=1)
        grad = halves(dot(do_ref[:, head * dv : (head + 1) * dv], up, 0, 0))
        decay = jnp.broadcast_to(jnp.exp(total[-1:]), (PAD, dk))
        for part in range(parts):
            grad_ref[head * parts + part] = grad[part * sub : (part + 1) * sub]
            decay_ref[head * parts + part] = decay
    for number in range(team):
        units = pl.ds((place_ref[0] ^ number) * per_owner, per_owner)
        outs[number][:, :sub] = grad_ref[units]
        outs[number][:, sub:] = decay_ref[units]


def local_kernel(*refs):
    for head in range(refs[5].shape[1]):
        local_head(head, *refs)


def local_head(
    head, g_ref, q_ref, k_ref, v_ref, do_ref, s_ref, dq_ref, dk_ref, dv_ref, terms_ref, fading_ref, sum_ref, added_ref
):
    dk_size, dv_size = s_ref.shape[2:]
    keys = slice(head * dk_size, (head + 1) * dk_size)
    values = slice(head * dv_size, (head + 1) * dv_size)
    length = g_ref.shape[0]
    total = running_sum(g_ref[:, keys])
    q = q_ref[:, keys].astype(f32)
    k = k_ref[:, keys].astype(f32)
    v = v_ref[:, values]
    do = do_ref[:, values]
    from_state = halves(dot(do, jnp.concatenate(split(s_ref[0, head]), axis=0), 1, 1))
    dq_all = jnp.exp(total) * from_state
    dots = split(jnp.where(at_or_after(length, length), dot(do, v, 1, 1), 0.0))
    flipped = split(jnp.where(at_or_before(length, length), dot(v, do, 1, 1), 0.0))
    dq = []
    dk = [0.0] * (length // CHUNK)
    dv = [0.0] * (length // CHUNK)
    for number in range(length // CHUNK):
        start, end = number * CHUNK, (number + 1) * CHUNK
        middle = total[start + CHUNK // 2 - 1 : start + CHUNK // 2]
        grow = jnp.exp(total[start:end] - middle)
        fade = jnp.exp(middle - total[:end])
        q_hi, q_lo = split(q[start:end] * grow)
        k_hi, k_lo = split(k[:end] * fade)
        dq.append(
            dq_all[start:end]
            + grow
            * (
                halves(dot(dots[0][start:end, :end], jnp.concatenate([k_hi, k_lo], axis=1), 1, 0))
                + dot(dots[1][start:end, :end], k_hi, 1, 0)
            )
        )
        dk_more = fade * (
            halves(dot(flipped[0][:end, start:end], jnp.concatenate([q_hi, q_lo], axis=1), 1, 0))
            + dot(flipped[1][:end, start:end], q_hi, 1, 0)
        )
        scores = dot(jnp.concatenate([k_hi, k_lo], axis=1), jnp.concatenate([q_hi, q_hi], axis=1), 1, 1)
        scores = scores + dot(k_hi, q_lo, 1, 1)
        seen = lax.broadcasted_iota(jnp.int32, (end, CHUNK), 0) <= start + lax.broadcasted_iota(
            jnp.int32, (end, CHUNK), 1
        )
        pair = jnp.concatenate(split(jnp.where(seen, scores, 0.0)), axis=1)
        dv_more = dot(pair, jnp.concatenate([do[start:end], do[start:end]], axis=0), 1, 0)
        for early in range(number + 1):
            rows = slice(early * CHUNK, (early + 1) * CHUNK)
            dk[early] = dk[early] + dk_more[rows]
            dv[early] = dv[early] + dv_more[rows]
    dq = jnp.concatenate(dq, axis=0)
    dk = jnp.concatenate(dk, axis=0)
    dq_ref[:, keys] = dq.astype(bf16)
    dk_ref[:, keys] = dk
    dv_ref[:, values] = jnp.concatenate(dv, axis=0)
    terms = q * dq - k * dk
    terms_ref[:, keys] = terms
    sum_ref[:, keys] = jnp.sum(terms, axis=0, keepdims=True)
    fading = jnp.exp(total[-1:] - total)
    fading_ref[:, keys] = fading
    added_ref[head] = halves(dot(v, jnp.concatenate(split(k * fading), axis=1), 0, 0))


def team_total_kernel(team, place_ref, *refs):
    pieces, out_ref = refs[:team], refs[team]
    sub = out_ref.shape[1] - PAD
    for place in range(team):

        @pl.when(place_ref[0] == place)
        def _():
            order = [pieces[member ^ place] for member in range(team)]
            for inner in range(out_ref.shape[0]):
                decays = [ref[inner, sub:] for ref in order]
                whole = decays[0]
                for decay in decays[1:]:
                    whole = whole * decay
                out_ref[inner, sub:] = whole

                def rows(step, _):
                    at = pl.ds(pl.multiple_of(step * PAD, PAD), PAD)
                    state = order[-1][inner, at]
                    for ref, decay in zip(order[-2::-1], decays[-2::-1]):
                        state = ref[inner, at] + decay * state
                    out_ref[inner, at] = state
                    return 0

                lax.fori_loop(0, sub // PAD, rows, 0, unroll=4)


def team_carry_kernel(team, place_ref, *refs):
    pieces, behind_ref, outs = refs[:team], refs[team], refs[team + 1 :]
    sub = outs[0].shape[1]
    for place in range(team):

        @pl.when(place_ref[0] == place)
        def _():
            order = [pieces[member ^ place] for member in range(team)]
            targets = [outs[member ^ place] for member in range(team)]
            for inner in range(outs[0].shape[0]):
                decays = [ref[inner, sub:] for ref in order]

                def rows(step, _):
                    at = pl.ds(pl.multiple_of(step * PAD, PAD), PAD)
                    state = behind_ref[inner, at]
                    for member in range(team - 1, -1, -1):
                        targets[member][inner, at] = state
                        if member:
                            state = order[member][inner, at] + decays[member] * state
                    return 0

                lax.fori_loop(0, sub // PAD, rows, 0, unroll=4)


def sum_kernel(team, place_ref, added_ref, sum_ref, *refs):
    pieces, (state_ref, out_ref) = refs[:team], refs[team:]
    per_owner, sub, dk = pieces[0].shape
    for number in range(team):
        state_ref[pl.ds((place_ref[0] ^ number) * per_owner, per_owner)] = pieces[number][...]
    heads, dv, _ = added_ref.shape
    parts = dv // sub
    for head in range(heads):
        less = 0.0
        for part in range(parts):
            product = state_ref[head * parts + part] * added_ref[head, part * sub : (part + 1) * sub]
            less = less + jnp.sum(product, axis=0, keepdims=True)
        keys = slice(head * dk, (head + 1) * dk)
        out_ref[:, keys] = sum_ref[:, keys] - less


def key_kernel(k_ref, v_ref, state_ref, dk_ref, terms_ref, fading_ref, out_ref, later_ref):
    heads, dv, dk = state_ref.shape
    for head in range(heads):
        keys = slice(head * dk, (head + 1) * dk)
        v = v_ref[:, head * dv : (head + 1) * dv]
        more = fading_ref[:, keys] * halves(dot(v, jnp.concatenate(split(state_ref[head]), axis=1), 1, 0))
        out_ref[:, keys] = (dk_ref[:, keys] + more).astype(bf16)
        later_ref[:, keys] = later_sum(terms_ref[:, keys] - k_ref[:, keys].astype(f32) * more)


def value_kernel(k_ref, fading_ref, state_ref, dv_ref, out_ref):
    heads, dv, dk = state_ref.shape
    for head in range(heads):
        keys = slice(head * dk, (head + 1) * dk)
        values = slice(head * dv, (head + 1) * dv)
        s_hi, s_lo = split(state_ref[head])
        k_hi, k_lo = split(k_ref[:, keys].astype(f32) * fading_ref[:, keys])
        more = dot(jnp.concatenate([k_hi, k_lo], axis=1), jnp.concatenate([s_hi, s_hi], axis=1), 1, 1)
        more = more + dot(k_hi, s_lo, 1, 1)
        out_ref[:, values] = (dv_ref[:, values] + more).astype(bf16)


def gate_kernel(dk, later_ref, behind_ref, g_ref, up_ref, gate_ref, latent_ref):
    part = 0.0
    for head in range(g_ref.shape[1] // dk):
        keys = slice(head * dk, (head + 1) * dk)
        grad = later_ref[:, keys] + behind_ref[:, keys]
        gate_ref[:, keys] = grad
        x_hi, x_lo = split(grad * ((1.0 - jnp.exp(16.0 * g_ref[:, keys])) / 16.0))
        u_hi, u_lo = split(up_ref[:, keys])
        part = part + dot(u_hi, x_hi, 1, 1) + dot(u_hi, x_lo, 1, 1) + dot(u_lo, x_hi, 1, 1)

    @pl.when(pl.program_id(0) == 0)
    def _():
        latent_ref[...] = part

    @pl.when(pl.program_id(0) > 0)
    def _():
        latent_ref[...] += part


def whole(shape):
    return pl.BlockSpec(shape, lambda *_: (0,) * len(shape))


def struct(shape, dtype=f32):
    return jax.ShapeDtypeStruct(shape, dtype)


def call(kernel, grid, in_specs, out_specs, out_shape, flops, scratch=()):
    return pl.pallas_call(
        kernel,
        grid=grid,
        in_specs=in_specs,
        out_specs=out_specs,
        out_shape=out_shape,
        scratch_shapes=list(scratch),
        cost_estimate=pl.CostEstimate(flops=flops, bytes_accessed=4 * 1024 * 1024, transcendentals=0),
        compiler_params=pltpu.CompilerParams(
            dimension_semantics=("arbitrary",) * len(grid), vmem_limit_bytes=16 * 1024 * 1024
        ),
    )


def exclusive_suffix(value, axis):
    count = lax.axis_size(axis)
    mine = lax.axis_index(axis)
    total, later = value, jnp.zeros_like(value)
    stride = 1
    while stride < count:
        perm = [(m, m ^ stride) for m in range(count)]
        other = lax.ppermute(total, axis, perm)
        later = jnp.where((mine & stride) == 0, later + other, later)
        total = total + other
        stride *= 2
    return later


def per_device(queries, keys, values, out_grad, log_gates, boundary_states, gate_up):
    count = lax.axis_size("seq")
    length, width = queries.shape
    _, heads, dk, dv = boundary_states.shape
    rank = gate_up.shape[0]
    team = math.gcd(TEAM, count)
    parts = team // math.gcd(heads, team)
    per_owner = heads * parts // team
    sub = dv // parts
    place = (lax.axis_index("seq") % team).astype(jnp.int32).reshape(1)
    smem = pl.BlockSpec(memory_space=pltpu.SMEM)
    unit = 2 * length * dv * 256 * heads

    piece = (per_owner, sub + PAD, dk)
    pieces = call(
        functools.partial(opening_kernel, team, parts),
        (1,),
        [smem, whole((length, width)), whole((length, width)), whole((length, heads * dv))],
        [whole(piece)] * team,
        [struct(piece)] * team,
        4 * unit,
        [pltpu.VMEM((heads * parts, sub, dk), f32), pltpu.VMEM((heads * parts, PAD, dk), f32)],
    )(place, log_gates, queries, out_grad)

    pairs = math.gcd(heads, 2)
    narrow = pl.BlockSpec((length, pairs * dk), lambda h: (0, h))
    wide = pl.BlockSpec((length, pairs * dv), lambda h: (0, h))
    row = pl.BlockSpec((1, pairs * dk), lambda h: (0, h))
    state_block = pl.BlockSpec((pairs, dv, dk), lambda h: (h, 0, 0))
    query_grad, dk_part, dv_part, terms, fading, sums, added = call(
        local_kernel,
        (heads // pairs,),
        [narrow, narrow, narrow, wide, wide, pl.BlockSpec((1, pairs, dk, dv), lambda h: (0, h, 0, 0))],
        [narrow, narrow, wide, narrow, narrow, row, state_block],
        [
            struct((length, width), bf16),
            struct((length, width)),
            struct((length, heads * dv)),
            struct((length, width)),
            struct((length, width)),
            struct((1, width)),
            struct((heads, dv, dk)),
        ],
        16 * unit,
    )(log_gates, queries, keys, values, out_grad, boundary_states)

    def exchange(blocks):
        moved = [blocks[0]]
        for number in range(1, team):
            moved.append(lax.ppermute(blocks[number], "seq", [(m, m ^ number) for m in range(count)]))
        return moved

    pieces = exchange(pieces)
    total = call(
        functools.partial(team_total_kernel, team),
        (1,),
        [smem] + [whole(piece)] * team,
        whole(piece),
        struct(piece),
        unit // 8,
    )(place, *pieces)
    behind = lax.ppermute(total, "seq", [(m, m - team) for m in range(team, count)])
    step = 1
    while step < count // team - 1:
        further = lax.ppermute(behind, "seq", [(m, m - team * step) for m in range(team * step, count)])
        decay = behind[:, sub : sub + 1]
        behind = jnp.concatenate(
            [behind[:, :sub] + decay * further[:, :sub], behind[:, sub:] * further[:, sub:]], axis=1
        )
        step *= 2
    carries = call(
        functools.partial(team_carry_kernel, team),
        (1,),
        [smem] + [whole(piece)] * (team + 1),
        [whole((per_owner, sub, dk))] * team,
        [struct((per_owner, sub, dk))] * team,
        unit // 8,
    )(place, *pieces, behind)
    carries = exchange(carries)

    state, sums = call(
        functools.partial(sum_kernel, team),
        (1,),
        [smem, whole((heads, dv, dk)), whole((1, width))] + [whole((per_owner, sub, dk))] * team,
        [whole((heads * parts, sub, dk)), whole((1, width))],
        [struct((heads * parts, sub, dk)), struct((1, width))],
        unit // 8,
    )(place, added, sums, *carries)
    state = state.reshape(heads, dv, dk)
    steps = math.gcd(heads, 2)
    some = heads // steps
    some_narrow = pl.BlockSpec((length, some * dk), lambda h: (0, h))
    some_wide = pl.BlockSpec((length, some * dv), lambda h: (0, h))
    some_state = pl.BlockSpec((some, dv, dk), lambda h: (h, 0, 0))

    key_grad, later = call(
        key_kernel,
        (steps,),
        [some_narrow, some_wide, some_state, some_narrow, some_narrow, some_narrow],
        [some_narrow, some_narrow],
        [struct((length, width), bf16), struct((length, width))],
        4 * unit,
    )(keys, values, state, dk_part, terms, fading)

    value_grad = call(
        value_kernel,
        (steps,),
        [some_narrow, some_narrow, some_state, some_wide],
        some_wide,
        struct((length, heads * dv), bf16),
        4 * unit,
    )(keys, fading, state, dv_part)

    behind_sum = exclusive_suffix(sums, "seq")
    gate_grad, latent = call(
        functools.partial(gate_kernel, dk),
        (steps,),
        [
            some_narrow,
            pl.BlockSpec((1, some * dk), lambda h: (0, h)),
            some_narrow,
            pl.BlockSpec((rank, some * dk), lambda h: (0, h)),
        ],
        [some_narrow, whole((rank, length))],
        [struct((length, width)), struct((rank, length))],
        unit,
    )(later, behind_sum, log_gates, gate_up)
    if lax.axis_size("head") == 2:
        latent = latent + lax.ppermute(latent, "head", [(0, 1), (1, 0)])
    else:
        latent = lax.psum(latent, "head")
    return query_grad, key_grad, value_grad, gate_grad, latent


def solution(mesh):
    return jax.shard_map(
        per_device,
        mesh=mesh,
        in_specs=(
            P("seq", "head"),
            P("seq", "head"),
            P("seq", "head"),
            P("seq", "head"),
            P("seq", "head"),
            P("seq", "head", None, None),
            P(None, "head"),
        ),
        out_specs=(
            P("seq", "head"),
            P("seq", "head"),
            P("seq", "head"),
            P("seq", "head"),
            P(None, "seq"),
        ),
        check_vma=False,
    )
```
